32 devices in a mesh: parts: 2 (over y), seq: 16 (over z, x, core).
Axes of the slice: x: 2, y: 2, z: 4, core: 2. Of those that a mesh axis runs over, the one named last changes fastest.
Arguments:
- queries: float32 [4096, 4096], P(('parts', 'seq')), parts along dimension 0, may hold values from -11 to 11
- visual_keys: float32 [4096, 512], P(('parts', 'seq')), parts along dimension 0, may hold values from -4 to 4
- visual_value_rows: float32 [4096, 512], P(('parts', 'seq')), parts along dimension 0, may hold values from -6 to 6
- output_gradient: float32 [4096, 4096], P(('parts', 'seq')), parts along dimension 0, may hold values from -6 to 6
- query_head_gate: float32 [32], replicated, may hold values from 0.3 to 2
- window_lists: int32 [2, 6], P('parts'), parts along dimension 0, may hold values from 0 to 15, as said below
- block_place: int32 [32], P('parts'), parts along dimension 0, may hold values from 0 to 15, each once
Outputs:
- output: float32 [4096, 4096], P(('parts', 'seq')), parts along dimension 0
- grad_queries: float32 [4096, 4096], P(('parts', 'seq')), parts along dimension 0
- grad_keys: float32 [4096, 512], P(('parts', 'seq')), parts along dimension 0
- grad_values: float32 [4096, 512], P(('parts', 'seq')), parts along dimension 0
The draws below stay inside these ranges and needn't reach their ends.
There are 2 independent parts, one for each index of `parts`. The reference program is written for one: setup_inputs(seed, part) draws one part's arguments, and reference() takes and returns one part's arrays. A program takes and returns all parts, laid end to end along the dimension named above; an argument that names none is the same for every part. Nothing has to cross between parts.
Inputs may be any that keep to these rules, and one draw needn't show every extreme that they name: `window_lists`: each row names 6 different visual blocks.
All inputs are finite; a program needn't handle non-finite values.
Results may differ from the reference program's by a relative error of at most 0.0003.
Values sent between devices are 32-bit elements; how exact they have to be, the bound alone decides.
No kernel may reach another device: no remote copies, remote signals or barrier semaphores. Data moves between devices by JAX's collectives and lax.ppermute only.
A program may use at most 128 MiB of HBM per device.

```python
import jax
import jax.numpy as jnp
from jax import lax

QUERY_HEADS = 32
KEY_VALUE_HEADS = 4
HEAD_FEATURES = 128
BLOCK_TOKENS = 128
LISTED_BLOCKS = 6
WINDOW_ROWS = 2048
TEXT = 2048
WINDOWS = 1
VBLOCKS = 16
VISUAL_TOKENS = 2048


def draw_visual_keys(key, part):
    gaussian_draw = jax.random.normal(jax.random.fold_in(key, 3), (VISUAL_TOKENS, KEY_VALUE_HEADS * HEAD_FEATURES), jnp.float32)
    return jnp.clip(gaussian_draw, -4.0, 4.0)


def draw_queries(key, part):
    gaussian_draw = jax.random.normal(jax.random.fold_in(key, 6), (TEXT, QUERY_HEADS * HEAD_FEATURES), jnp.float32)
    return jnp.clip(gaussian_draw, -4.0, 4.0)


def draw_window_lists(key, part):
    raw_scores = jax.random.randint(jax.random.fold_in(key, 4711), (WINDOWS, VBLOCKS), 0, 1 << 20, jnp.int32)
    distinct_scores = raw_scores * VBLOCKS + jnp.arange(VBLOCKS, dtype=jnp.int32)[None, :]
    ranking = jnp.argsort(-distinct_scores, axis=1, stable=True)
    return ranking[:, :LISTED_BLOCKS].astype(jnp.int32)


def levels(own_key, shape, pieces, low, high):
    loudness = 1.0
    for axis_at, blocks in pieces:
        draws = jax.random.uniform(jax.random.fold_in(jax.random.fold_in(own_key, 6), axis_at), (blocks,), jnp.float32, low / len(pieces), high / len(pieces))
        loudness = loudness * jnp.repeat(jnp.exp(draws), shape[axis_at] // blocks).reshape((-1,) + (1,) * (len(shape) - 1 - axis_at))
    return loudness


def normal_values(own_key, extent, spread, most, shards=(), held_as=jnp.bfloat16):
    loudness = levels(own_key, extent, shards, -0.22, 0.18) if shards else 1.0
    values = jax.random.normal(own_key, extent, jnp.float32) * spread * loudness
    return jnp.minimum(jnp.maximum(values, -most), most).astype(held_as)


def setup_inputs(seed: int = 0, part: int = 0) -> dict:
    seeds = jax.random.split(jax.random.key(seed), 8)
    own_keys = jax.random.split(jax.random.fold_in(seeds[7], part), 8)
    queries = draw_queries(jax.random.fold_in(jax.random.fold_in(seeds[7], part), 71), part)
    visual_keys = draw_visual_keys(jax.random.fold_in(jax.random.fold_in(seeds[7], part), 71), part)
    visual_value_rows = normal_values(own_keys[2], (VISUAL_TOKENS, KEY_VALUE_HEADS * HEAD_FEATURES), 1.0, 6.0, ((0, 16),), jnp.float32)
    output_gradient = normal_values(own_keys[3], (TEXT, QUERY_HEADS * HEAD_FEATURES), 1.0, 6.0, ((0, 16),), jnp.float32)
    query_head_gate = jnp.clip(jax.random.uniform(seeds[4], (QUERY_HEADS,), jnp.float32, 0.3, 2.0), 0.3, 2.0)
    window_lists = draw_window_lists(jax.random.fold_in(jax.random.fold_in(seeds[7], part), 71), part)
    block_place = jax.random.permutation(own_keys[6], VBLOCKS).astype(jnp.int32)
    return dict(queries=queries, visual_keys=visual_keys, visual_value_rows=visual_value_rows, output_gradient=output_gradient, query_head_gate=query_head_gate, window_lists=window_lists, block_place=block_place)


HIGHEST = lax.Precision.HIGHEST


def attend(window_query_rows, window_key_rows, window_value_rows, gradient_rows, gate_lookup):
    inverse_root = HEAD_FEATURES ** -0.5
    scores = jnp.einsum('rkgd,skd->kgrs', window_query_rows, window_key_rows, precision=HIGHEST) * inverse_root
    row_max = jnp.max(scores, axis=-1, keepdims=True)
    raised = jnp.exp(scores - row_max)
    weights = raised / jnp.sum(raised, axis=-1, keepdims=True)
    attended = jnp.einsum('kgrs,skd->rkgd', weights, window_value_rows, precision=HIGHEST)
    output = attended * gate_lookup[None, :, :, None]
    grad_attended = gradient_rows * gate_lookup[None, :, :, None]
    row_dot = jnp.einsum('rkgd,rkgd->kgr', grad_attended, attended, precision=HIGHEST)
    grad_weights = jnp.einsum('rkgd,skd->kgrs', grad_attended, window_value_rows, precision=HIGHEST)
    grad_scores = weights * (grad_weights - row_dot[..., None])
    grad_query = jnp.einsum('kgrs,skd->rkgd', grad_scores, window_key_rows, precision=HIGHEST) * inverse_root
    grad_key = jnp.einsum('kgrs,rkgd->skd', grad_scores, window_query_rows, precision=HIGHEST) * inverse_root
    grad_value = jnp.einsum('kgrs,rkgd->skd', weights, grad_attended, precision=HIGHEST)
    return output, grad_query, grad_key, grad_value


def reference(queries, visual_keys, visual_value_rows, output_gradient, query_head_gate, window_lists, block_place):
    queries_per_group = QUERY_HEADS // KEY_VALUE_HEADS
    feature_width = KEY_VALUE_HEADS * HEAD_FEATURES
    gate_lookup = jnp.tanh(query_head_gate).reshape(KEY_VALUE_HEADS, queries_per_group)
    gathered_key_block = visual_keys.reshape(VBLOCKS, BLOCK_TOKENS, feature_width)
    gathered_value_block = visual_value_rows.reshape(VBLOCKS, BLOCK_TOKENS, feature_width)
    window_count = TEXT // WINDOW_ROWS

    def one_window(window_index):
        picked_blocks = block_place[window_lists[window_index]]
        window_key_rows = gathered_key_block[picked_blocks].reshape(LISTED_BLOCKS * BLOCK_TOKENS, KEY_VALUE_HEADS, HEAD_FEATURES)
        window_value_rows = gathered_value_block[picked_blocks].reshape(LISTED_BLOCKS * BLOCK_TOKENS, KEY_VALUE_HEADS, HEAD_FEATURES)
        block_start = (window_index * WINDOW_ROWS).astype(jnp.int32)
        window_query_rows = lax.dynamic_slice_in_dim(queries, block_start, WINDOW_ROWS, 0).reshape(WINDOW_ROWS, KEY_VALUE_HEADS, queries_per_group, HEAD_FEATURES)
        gradient_rows = lax.dynamic_slice_in_dim(output_gradient, block_start, WINDOW_ROWS, 0).reshape(WINDOW_ROWS, KEY_VALUE_HEADS, queries_per_group, HEAD_FEATURES)
        output, grad_query, grad_key, grad_value = attend(window_query_rows, window_key_rows, window_value_rows, gradient_rows, gate_lookup)
        return (output.reshape(WINDOW_ROWS, QUERY_HEADS * HEAD_FEATURES), grad_query.reshape(WINDOW_ROWS, QUERY_HEADS * HEAD_FEATURES),
                grad_key.reshape(LISTED_BLOCKS, BLOCK_TOKENS, feature_width), grad_value.reshape(LISTED_BLOCKS, BLOCK_TOKENS, feature_width))

    results = lax.map(one_window, jnp.arange(window_count, dtype=jnp.int32))
    output = results[0].reshape(TEXT, QUERY_HEADS * HEAD_FEATURES)
    grad_queries = results[1].reshape(TEXT, QUERY_HEADS * HEAD_FEATURES)
    chosen_all = block_place[window_lists].reshape(-1)
    grad_keys = jnp.zeros((VBLOCKS, BLOCK_TOKENS, feature_width), jnp.float32).at[chosen_all].add(
        results[2].reshape(-1, BLOCK_TOKENS, feature_width)).reshape(VISUAL_TOKENS, feature_width)
    grad_values = jnp.zeros((VBLOCKS, BLOCK_TOKENS, feature_width), jnp.float32).at[chosen_all].add(
        results[3].reshape(-1, BLOCK_TOKENS, feature_width)).reshape(VISUAL_TOKENS, feature_width)
    return output, grad_queries, grad_keys, grad_values
```

```python
import functools

import jax
import jax.numpy as jnp
from jax import lax
from jax.experimental import pallas as pl
from jax.experimental.pallas import tpu as pltpu
from jax.sharding import PartitionSpec as P

F = 128
BLOCK_TOKENS = 128
WINDOW_ROWS = 2048
CORES = 2
HEADS = 8
CHUNK = 128
LN2 = 0.6931471805599453
LOG2E = 1.4426950408889634
BF = jnp.bfloat16
F32 = jnp.float32


def split(x):
    high = x.astype(BF)
    return high, (x - high.astype(F32)).astype(BF)


def dot(a, b):
    return lax.dot_general(a, b, (((1,), (0,)), ((), ())), preferred_element_type=F32)


def kernel(n_in, groups, steps, keys, core_ref, gate_ref, qo_ref, qp_ref, go_ref, gp_ref, *rest):
    kv_in = rest[:n_in]
    oo_ref, op_ref, do_ref, dp_ref, dkv_ref = rest[n_in : n_in + 5]
    kv, kk, vv, kt, vt, s_ref, ph, plo, dh, dlo, dka, dva, sem = rest[n_in + 5 :]
    g, side, p = pl.program_id(0), pl.program_id(1), pl.program_id(2)
    inv_root = F ** (-0.5)
    half = groups * F

    @pl.when((g == 0) & (side == 0) & (p == 0))
    def _():
        copies, at = [], 0
        for i, src in enumerate(kv_in):
            rows = src.shape[0]
            copies.append(pltpu.make_async_copy(src, kv.at[pl.ds(at, rows)], sem.at[i]))
            at += rows
        for c in copies:
            c.start()
        for c in copies:
            c.wait()

    @pl.when((side == 0) & (p == 0))
    def _():
        for off, pack, tr in ((0, kk, kt), (half, vv, vt)):
            x = kv[:, pl.ds(pl.multiple_of(off + g * F, F), F)]
            high, low = split(x)
            pack[:, 0:F] = high
            pack[:, F : 2 * F] = low
            pack[:, 2 * F : 3 * F] = high
            pack[:, 3 * F : 4 * F] = low
            high, low = split(x.T)
            tr[0:F, :] = high
            tr[F : 2 * F, :] = low
        dka[...] = jnp.zeros_like(dka)
        dva[...] = jnp.zeros_like(dva)

    def pack_rows(own, other, scale):
        x = jnp.where(side == 0, own[...], other[...])
        xs = [x[:, h * F : (h + 1) * F] * scale(h) for h in range(HEADS)]
        rh, rl = split(jnp.concatenate(xs, axis=0))
        cols = jnp.concatenate([y.T for y in xs], axis=1)
        ch, cl = split(cols)
        return jnp.concatenate([rh, rl], axis=1), jnp.concatenate([ch, ch, cl, cl], axis=0), cols

    base = ((core_ref[0] * groups + g) * steps + p) * HEADS
    gates = [gate_ref[base + h] for h in range(HEADS)]
    qr, qc, _ = pack_rows(qo_ref, qp_ref, lambda h: inv_root * LOG2E)
    ar, ac, acols = pack_rows(go_ref, gp_ref, lambda h: gates[h])

    def put(own, other, values):
        @pl.when(side == 0)
        def _():
            for h, y in enumerate(values):
                own[:, h * F : (h + 1) * F] = y

        @pl.when(side != 0)
        def _():
            for h, y in enumerate(values):
                other[:, h * F : (h + 1) * F] = y

    tiles = [slice(c, c + CHUNK) for c in range(0, keys, CHUNK)]
    m = None
    for t in tiles:
        s = dot(kk[t, :], qc)
        s_ref[t, :] = s
        mc = jnp.max(s, axis=0, keepdims=True)
        m = mc if m is None else jnp.maximum(m, mc)
    l = None
    for t in tiles:
        e = jnp.exp2(s_ref[t, :] - m)
        s_ref[t, :] = e
        lc = jnp.sum(e, axis=0, keepdims=True)
        l = lc if l is None else l + lc
    inv = 1.0 / l
    for t in tiles:
        w = s_ref[t, :] * inv
        s_ref[t, :] = w
        ph[t, :], plo[t, :] = split(w)
    o2 = dot(vt[...], ph[...])
    ot = o2[0:F, :] + o2[F : 2 * F, :] + dot(vt[0:F, :], plo[...])
    delta = jnp.sum(ot * acols, axis=0, keepdims=True)
    put(oo_ref, op_ref, [ot[:, h * F : (h + 1) * F].T * gates[h] for h in range(HEADS)])
    for t in tiles:
        dva[t, :] += dot(ph[t, :], ar) + dot(plo[t, :], ar)
    for t in tiles:
        ds = s_ref[t, :] * (dot(vv[t, :], ac) - delta)
        dh[t, :], dlo[t, :] = split(ds)
    for t in tiles:
        dka[t, :] += dot(dh[t, :], qr) + dot(dlo[t, :], qr)
    d2 = dot(kt[...], dh[...])
    dt = (d2[0:F, :] + d2[F : 2 * F, :] + dot(kt[0:F, :], dlo[...])) * inv_root
    put(do_ref, dp_ref, [dt[:, h * F : (h + 1) * F].T for h in range(HEADS)])

    @pl.when((side == pl.num_programs(1) - 1) & (p == steps - 1))
    def _():
        col = pl.multiple_of(g * F, F)
        dkv_ref[:, pl.ds(col, F)] = (dka[:, 0:F] + dka[:, F : 2 * F]) * LN2
        dkv_ref[:, pl.ds(pl.multiple_of(half + col, F), F)] = dva[:, 0:F] + dva[:, F : 2 * F]


def attend(core, gate, q_own, q_other, g_own, g_other, kv_in):
    rows = q_own.shape[0]
    width = kv_in[0].shape[1]
    groups = width // F // 2
    steps = q_other.shape[1] // F // groups // HEADS
    n_in = len(kv_in)
    keys = sum(x.shape[0] for x in kv_in)
    n = HEADS * rows
    blocks = groups * steps

    def own(g, side, p, c):
        return 0, c[0] * blocks + g * steps + jnp.where(side == 0, p, steps - 1)

    def other(g, side, p, c):
        return 0, g * steps + jnp.where(side == 0, 0, p)

    own_block = pl.BlockSpec((rows, HEADS * F), own)
    other_block = pl.BlockSpec((rows, HEADS * F), other)
    anywhere = pl.BlockSpec(memory_space=pl.ANY)
    full = jax.ShapeDtypeStruct(q_own.shape, F32)
    part = jax.ShapeDtypeStruct(q_other.shape, F32)
    spec = pltpu.PrefetchScalarGridSpec(
        num_scalar_prefetch=1,
        grid=(groups, 2, steps),
        in_specs=[pl.BlockSpec(memory_space=pltpu.SMEM), own_block, other_block, own_block, other_block]
        + [anywhere] * n_in,
        out_specs=[
            own_block,
            other_block,
            own_block,
            other_block,
            pl.BlockSpec((keys, width), lambda g, side, p, c: (0, 0)),
        ],
        scratch_shapes=[
            pltpu.VMEM((keys, width), F32),
            pltpu.VMEM((keys, 4 * F), BF),
            pltpu.VMEM((keys, 4 * F), BF),
            pltpu.VMEM((2 * F, keys), BF),
            pltpu.VMEM((2 * F, keys), BF),
            pltpu.VMEM((keys, n), F32),
            pltpu.VMEM((keys, n), BF),
            pltpu.VMEM((keys, n), BF),
            pltpu.VMEM((keys, n), BF),
            pltpu.VMEM((keys, n), BF),
            pltpu.VMEM((keys, 2 * F), F32),
            pltpu.VMEM((keys, 2 * F), F32),
            pltpu.SemaphoreType.DMA((n_in,)),
        ],
    )
    return pl.pallas_call(
        functools.partial(kernel, n_in, groups, steps, keys),
        out_shape=[full, part, full, part, jax.ShapeDtypeStruct((keys, width), F32)],
        grid_spec=spec,
        compiler_params=pltpu.CompilerParams(
            dimension_semantics=("arbitrary",) * 3, vmem_limit_bytes=56 << 20
        ),
        cost_estimate=pl.CostEstimate(
            flops=48 * rows * q_other.shape[1] * keys,
            bytes_accessed=32 * rows * q_other.shape[1],
            transcendentals=2 * rows * q_other.shape[1] // F * keys,
        ),
        name="attend",
    )(core, gate, q_own, q_other, g_own, g_other, *kv_in)


def ring_tables(devices, members):
    chips = members // CORES
    order = list(range(0, chips, 2)) + [c for c in range(chips - 1, 0, -1) if c % 2]
    right, left, pair = [], [], []
    for base in range(0, devices, members):
        for at, c in enumerate(order):
            after = order[(at + 1) % chips]
            for core in range(CORES):
                a, b = base + CORES * c + core, base + CORES * after + core
                right.append((a, b))
                left.append((b, a))
                pair.append((a, base + CORES * c + 1 - core))
    return chips, right, left, pair


def local(queries, visual_keys, visual_value_rows, output_gradient, query_head_gate, window_lists, block_place):
    row_count, q_width = queries.shape
    width = visual_keys.shape[1]
    list_len = window_lists.shape[1]
    devices = lax.axis_size("seq")
    members = WINDOW_ROWS // row_count
    windows = devices // members
    blocks_here = visual_keys.shape[0] // BLOCK_TOKENS
    positions = devices * blocks_here
    chips, right, left, pair = ring_tables(devices, members)
    piece = BLOCK_TOKENS // chips
    half_width, q_half = width // CORES, q_width // CORES
    far = chips // 2
    index = lax.axis_index("seq")
    core = index % CORES

    def shift(x, table):
        return lax.ppermute(x, "seq", table)

    mine = lax.dynamic_index_in_dim(window_lists, index // members, 0, keepdims=False)
    wanted = jnp.take(block_place, mine, axis=0)

    def theirs(x):
        return shift(lax.dynamic_slice_in_dim(x, (1 - core) * q_half, q_half, 1), pair)

    def by_core(x):
        x = x.reshape(blocks_here, chips, piece, CORES, half_width)
        return x.transpose(0, 1, 3, 2, 4)

    x = jnp.concatenate([by_core(visual_keys), by_core(visual_value_rows)], axis=-1)
    x = x.reshape(blocks_here, members, piece, width)
    x = jnp.tile(x, (1, windows, 1, 1))
    x = lax.all_to_all(x, "seq", split_axis=1, concat_axis=0, tiled=True)
    q_other, g_other = theirs(queries), theirs(output_gradient)
    x = jnp.take(x.reshape(positions, piece, width), wanted, axis=0).reshape(list_len * piece, width)

    n = x.shape[0]
    cut = n // 2
    rights, lefts = [], []
    r = l = x
    for step in range(1, far + 1):
        if step == far:
            r, l = r[:cut], l[cut:]
        r, l = shift(r, right), shift(l, left)
        rights.append(r)
        lefts.append(l)
    chunks = [x] + rights + lefts
    gate = jnp.tanh(query_head_gate)
    out_own, out_other, dq_own, dq_other, dkv = attend(
        core.reshape(1), gate, queries, q_other, output_gradient, g_other, chunks
    )
    parts, at = [], 0
    for c in chunks:
        parts.append(dkv[at : at + c.shape[0]])
        at += c.shape[0]
    rights, lefts = parts[1 : 1 + far], parts[1 + far :]
    r, l = shift(rights[-1], left), shift(lefts[-1], right)
    for step in range(far - 1, 0, -1):
        a, b = rights[step - 1], lefts[step - 1]
        if step == far - 1:
            a = jnp.concatenate([a[:cut] + r, a[cut:]], axis=0)
            b = jnp.concatenate([b[:cut], b[cut:] + l], axis=0)
        else:
            a, b = a + r, b + l
        r, l = shift(a, left), shift(b, right)
    out_back, dq_back = shift(out_other, pair), shift(dq_other, pair)
    total = (parts[0] + r + l).reshape(list_len, piece, width)
    hit = wanted[None, :] == jnp.arange(positions, dtype=jnp.int32)[:, None]
    slot = jnp.argmax(hit, axis=1)
    sent = jnp.where(jnp.any(hit, axis=1)[:, None, None], jnp.take(total, slot, axis=0), 0.0)
    back = lax.all_to_all(
        sent.reshape(devices, blocks_here, piece, width), "seq", split_axis=0, concat_axis=0, tiled=True
    ).reshape(windows, chips, CORES, blocks_here, piece, width)
    back = back[0] if windows == 1 else jnp.sum(back, axis=0)

    def by_rows(x):
        return x.transpose(2, 0, 3, 1, 4).reshape(blocks_here * BLOCK_TOKENS, width)

    def whole(x, y):
        return lax.dynamic_update_slice_in_dim(x, y, (1 - core) * q_half, 1)

    return (
        whole(out_own, out_back),
        whole(dq_own, dq_back),
        by_rows(back[..., :half_width]),
        by_rows(back[..., half_width:]),
    )


def solution(mesh):
    rows = P(("parts", "seq"), None)
    return jax.shard_map(
        local,
        mesh=mesh,
        in_specs=(rows, rows, rows, rows, P(), P("parts", None), P("parts")),
        out_specs=(rows, rows, rows, rows),
        check_vma=False,
    )
```

```python
import functools

import jax
import jax.numpy as jnp
from jax import lax
from jax.experimental import pallas as pl
from jax.experimental.pallas import tpu as pltpu
from jax.sharding import PartitionSpec as P


F = 128
BLOCK_TOKENS = 128
WINDOW_ROWS = 2048
CORES = 2
HEADS = 8
CHUNK = 256
VMEM_LIMIT = 32 << 20
LN2 = 0.6931471805599453
LOG2E = 1.4426950408889634
BF = jnp.bfloat16
F32 = jnp.float32


def split(x):
    high = x.astype(BF)
    return high, (x - high.astype(F32)).astype(BF)


def dot(a, b):
    return lax.dot_general(a, b, (((1,), (0,)), ((), ())), preferred_element_type=F32)


def kernel(n_in, groups, steps, keys, gate_ref, q_ref, g_ref, *rest):
    kv_in = rest[:n_in]
    out_ref, dq_ref = rest[n_in : n_in + 2]
    dkv_out = rest[n_in + 2 : 2 * n_in + 2]
    kv, kk, vv, kt, vt, s_ref, d_ref, ph, plo, dh, dlo, dka, dva, sem = rest[2 * n_in + 2 :]
    g, side, p = pl.program_id(0), pl.program_id(1), pl.program_id(2)
    inv_root = F ** (-0.5)
    half = groups * F

    @pl.when((g == 0) & (side == 0) & (p == 0))
    def _():
        copies, at = [], 0
        for i, src in enumerate(kv_in):
            rows = src.shape[0]
            copies.append(pltpu.make_async_copy(src, kv.at[pl.ds(at, rows)], sem.at[i]))
            at += rows
        for c in copies:
            c.start()
        for c in copies:
            c.wait()

    @pl.when((side == 0) & (p == 0))
    def _():
        for off, pack, tr in ((0, kk, kt), (half, vv, vt)):
            x = kv[:, pl.ds(pl.multiple_of(off + g * F, F), F)]
            high, low = split(x)
            pack[:, 0:F] = high
            pack[:, F : 2 * F] = low
            pack[:, 2 * F : 3 * F] = high
            pack[:, 3 * F : 4 * F] = low
            high, low = split(x.T)
            tr[0:F, :] = high
            tr[F : 2 * F, :] = low
        dka[...] = jnp.zeros_like(dka)
        dva[...] = jnp.zeros_like(dva)

    def pack_rows(ref, scale):
        xs = [ref[:, h * F : (h + 1) * F] * scale(h) for h in range(HEADS)]
        rh, rl = split(jnp.concatenate(xs, axis=0))
        cols = jnp.concatenate([y.T for y in xs], axis=1)
        ch, cl = split(cols)
        return jnp.concatenate([rh, rl], axis=1), jnp.concatenate([ch, ch, cl, cl], axis=0), cols

    base = (g * steps + p) * HEADS
    gates = [gate_ref[base + h] for h in range(HEADS)]
    qr, qc, _ = pack_rows(q_ref, lambda h: inv_root * LOG2E)
    ar, ac, acols = pack_rows(g_ref, lambda h: gates[h])

    tiles = [slice(c, c + CHUNK) for c in range(0, keys, CHUNK)]
    m = None
    for t in tiles:
        s = dot(kk[t, :], qc)
        s_ref[t, :] = s
        mc = jnp.max(s, axis=0, keepdims=True)
        m = mc if m is None else jnp.maximum(m, mc)
    l = None
    for t in tiles:
        d_ref[t, :] = dot(vv[t, :], ac)
        e = jnp.exp2(s_ref[t, :] - m)
        s_ref[t, :] = e
        lc = jnp.sum(e, axis=0, keepdims=True)
        l = lc if l is None else l + lc
    inv = 1.0 / l
    for t in tiles:
        w = s_ref[t, :] * inv
        s_ref[t, :] = w
        ph[t, :], plo[t, :] = split(w)
        dva[t, :] += dot(ph[t, :], ar) + dot(plo[t, :], ar)
    o2 = dot(vt[...], ph[...])
    ot = o2[0:F, :] + o2[F : 2 * F, :] + dot(vt[0:F, :], plo[...])
    delta = jnp.sum(ot * acols, axis=0, keepdims=True)
    for t in tiles:
        ds = s_ref[t, :] * (d_ref[t, :] - delta)
        dh[t, :], dlo[t, :] = split(ds)
        dka[t, :] += dot(dh[t, :], qr) + dot(dlo[t, :], qr)
    for h in range(HEADS):
        out_ref[:, h * F : (h + 1) * F] = ot[:, h * F : (h + 1) * F].T * gates[h]
    d2 = dot(kt[...], dh[...])
    dt = (d2[0:F, :] + d2[F : 2 * F, :] + dot(kt[0:F, :], dlo[...])) * inv_root
    for h in range(HEADS):
        dq_ref[:, h * F : (h + 1) * F] = dt[:, h * F : (h + 1) * F].T

    @pl.when((side == pl.num_programs(1) - 1) & (p == steps - 1))
    def _():
        col = pl.multiple_of(g * F, F)
        dk = (dka[:, 0:F] + dka[:, F : 2 * F]) * LN2
        dv = dva[:, 0:F] + dva[:, F : 2 * F]
        at = 0
        for ref in dkv_out:
            rows = ref.shape[0]
            ref[:, pl.ds(col, F)] = dk[at : at + rows]
            ref[:, pl.ds(pl.multiple_of(half + col, F), F)] = dv[at : at + rows]
            at += rows


def attend(gate, q, go, kv_in):
    sides = CORES
    rows = q.shape[0] // sides
    width = kv_in[0].shape[1]
    groups = width // F // 2
    steps = q.shape[1] // F // groups // HEADS
    n_in = len(kv_in)
    keys = sum(x.shape[0] for x in kv_in)
    n = HEADS * rows
    block = pl.BlockSpec((rows, HEADS * F), lambda g, side, p: (side, g * steps + p))
    like = jax.ShapeDtypeStruct(q.shape, F32)
    return pl.pallas_call(
        functools.partial(kernel, n_in, groups, steps, keys),
        out_shape=[like, like] + [jax.ShapeDtypeStruct(x.shape, F32) for x in kv_in],
        grid=(groups, sides, steps),
        in_specs=[pl.BlockSpec(memory_space=pltpu.SMEM), block, block]
        + [pl.BlockSpec(memory_space=pl.ANY)] * n_in,
        out_specs=[block, block] + [pl.BlockSpec(x.shape, lambda g, side, p: (0, 0)) for x in kv_in],
        scratch_shapes=[
            pltpu.VMEM((keys, width), F32),
            pltpu.VMEM((keys, 4 * F), BF),
            pltpu.VMEM((keys, 4 * F), BF),
            pltpu.VMEM((2 * F, keys), BF),
            pltpu.VMEM((2 * F, keys), BF),
            pltpu.VMEM((keys, n), F32),
            pltpu.VMEM((keys, n), F32),
            pltpu.VMEM((keys, n), BF),
            pltpu.VMEM((keys, n), BF),
            pltpu.VMEM((keys, n), BF),
            pltpu.VMEM((keys, n), BF),
            pltpu.VMEM((keys, 2 * F), F32),
            pltpu.VMEM((keys, 2 * F), F32),
            pltpu.SemaphoreType.DMA((n_in,)),
        ],
        compiler_params=pltpu.CompilerParams(
            dimension_semantics=("arbitrary",) * 3, vmem_limit_bytes=VMEM_LIMIT
        ),
        cost_estimate=pl.CostEstimate(
            flops=24 * q.size * keys,
            bytes_accessed=16 * q.size,
            transcendentals=q.size // F * keys,
        ),
        name="attend",
    )(gate, q, go, *kv_in)


def ring_tables(devices, members):
    chips = members // CORES
    order = list(range(0, chips, 2)) + [c for c in range(chips - 1, 0, -1) if c % 2]
    right, left, pair = [], [], []
    for base in range(0, devices, members):
        for at, c in enumerate(order):
            after = order[(at + 1) % chips]
            for core in range(CORES):
                a, b = base + CORES * c + core, base + CORES * after + core
                right.append((a, b))
                left.append((b, a))
                pair.append((a, base + CORES * c + 1 - core))
    return chips, right, left, pair


def local(queries, visual_keys, visual_value_rows, output_gradient, query_head_gate, window_lists, block_place):
    row_count, q_width = queries.shape
    width = visual_keys.shape[1]
    list_len = window_lists.shape[1]
    devices = lax.axis_size("seq")
    members = WINDOW_ROWS // row_count
    windows = devices // members
    blocks_here = visual_keys.shape[0] // BLOCK_TOKENS
    positions = devices * blocks_here
    chips, right, left, pair = ring_tables(devices, members)
    piece = BLOCK_TOKENS // chips
    half_width, q_half = width // CORES, q_width // CORES
    far = chips // 2
    index = lax.axis_index("seq")
    core = index % CORES

    def shift(x, table):
        return lax.ppermute(x, "seq", table)

    mine = lax.dynamic_index_in_dim(window_lists, index // members, 0, keepdims=False)
    wanted = jnp.take(block_place, mine, axis=0)

    def half(x, which):
        return lax.dynamic_slice_in_dim(x, which * q_half, q_half, 1)

    def both(x):
        mine, theirs = half(x, core), half(x, 1 - core)
        return jnp.concatenate([mine, shift(theirs, pair)], axis=0)

    def for_core(c):
        cols = slice(c * half_width, (c + 1) * half_width)
        x = jnp.concatenate([visual_keys[:, cols], visual_value_rows[:, cols]], axis=1)
        return x.reshape(blocks_here, chips, 1, piece, width)

    x = jnp.concatenate([for_core(c) for c in range(CORES)], axis=2).reshape(blocks_here, members, piece, width)
    x = jnp.tile(x, (1, windows, 1, 1))
    x, queries, output_gradient = lax.optimization_barrier((x, queries, output_gradient))
    x = lax.all_to_all(x, "seq", split_axis=1, concat_axis=0, tiled=True)
    q_both, g_both = both(queries), both(output_gradient)
    x = jnp.take(x.reshape(positions, piece, width), wanted, axis=0).reshape(list_len * piece, width)

    n = x.shape[0]
    cut = n // 2
    rights, lefts = [], []
    r = l = x
    for step in range(1, far + 1):
        if step == far:
            r, l = r[:cut], l[cut:]
        r, l = shift(r, right), shift(l, left)
        rights.append(r)
        lefts.append(l)
    chunks = [x] + rights + lefts
    gate = lax.dynamic_slice_in_dim(jnp.tanh(query_head_gate), core * (q_half // F), q_half // F, 0)
    out, dq, *parts = attend(gate, q_both, g_both, chunks)
    rights, lefts = parts[1 : 1 + far], parts[1 + far :]
    r, l = shift(rights[-1], left), shift(lefts[-1], right)
    for step in range(far - 1, 0, -1):
        r, l = lax.optimization_barrier((r, l))
        a, b = rights[step - 1], lefts[step - 1]
        if step == far - 1:
            a = jnp.concatenate([a[:cut] + r, a[cut:]], axis=0)
            b = jnp.concatenate([b[:cut], b[cut:] + l], axis=0)
        else:
            a, b = a + r, b + l
        a, b = lax.optimization_barrier((a, b))
        r, l = shift(a, left), shift(b, right)
    out_back, dq_back = shift(out[row_count:], pair), shift(dq[row_count:], pair)
    total = (parts[0] + r + l).reshape(list_len, piece, width)
    hit = wanted[None, :] == jnp.arange(positions, dtype=jnp.int32)[:, None]
    slot = jnp.argmax(hit, axis=1)
    sent = jnp.where(jnp.any(hit, axis=1)[:, None, None], jnp.take(total, slot, axis=0), 0.0)
    back = lax.all_to_all(
        sent.reshape(devices, blocks_here, piece, width), "seq", split_axis=0, concat_axis=0, tiled=True
    ).reshape(windows, chips, CORES, blocks_here, piece, width)
    back = back[0] if windows == 1 else jnp.sum(back, axis=0)

    def by_rows(x):
        return x.transpose(2, 0, 3, 1, 4).reshape(blocks_here * BLOCK_TOKENS, width)

    def whole(x, y):
        x = x[:row_count]
        return jnp.where(core == 0, jnp.concatenate([x, y], axis=1), jnp.concatenate([y, x], axis=1))

    return (
        whole(out, out_back),
        whole(dq, dq_back),
        by_rows(back[..., :half_width]),
        by_rows(back[..., half_width:]),
    )


def solution(mesh):
    rows = P(("parts", "seq"), None)
    return jax.shard_map(
        local,
        mesh=mesh,
        in_specs=(rows, rows, rows, rows, P(), P("parts", None), P("parts")),
        out_specs=(rows, rows, rows, rows),
        check_vma=False,
    )
```
